128 devices in a mesh: freq: 8 (over x, z_hi), panel: 16 (over z_lo, y, core).
Axes of the slice: x: 4, y: 4, z: 4 (z_hi: 2, z_lo: 2; z = z_hi * 2 + z_lo), core: 2. Of those that a mesh axis runs over, the one named last changes fastest.
Arguments:
- traces: bfloat16 [640, 640, 1024], P('panel', 'freq'), may hold values from -6 to 6
- filters: float32 [16, 7, 64], replicated, may hold values from -0.25 to 0.25
Outputs:
- primaries: bfloat16 [640, 640, 1024], P('panel', 'freq')
The draws below stay inside these ranges and needn't reach their ends.
All inputs are finite; a program needn't handle non-finite values.
Results may differ from the reference program's by a relative error of at most 0.0095.
Values may be sent and summed in bfloat16 or wider, within the bound.
No kernel may reach another device: no remote copies, remote signals or barrier semaphores. Data moves between devices by JAX's collectives and lax.ppermute only.
A program may use at most 128 MiB of HBM per device.

```python
import math
from functools import partial
import jax
import jax.numpy as jnp
from jax import lax

NS = 640
NR = 640
NT = 1024
NF = 96
FLO = 8
TAPS = 64
SPAN = 7
RWIN = 40
NWIN = 16


def block_scale(own_key, shape, shards, low, largest):
    factor_of, own = 1.0, jax.random.fold_in(own_key, 6)
    for axis_at, shards_of in shards:
        heights = jnp.exp(jax.random.uniform(jax.random.fold_in(own, axis_at), (shards_of,), jnp.float32, low / len(shards), largest / len(shards)))
        factor_of = factor_of * jnp.repeat(heights, shape[axis_at] // shards_of).reshape([-1 if axis == axis_at else 1 for axis in range(len(shape))])
    return factor_of


def bell_draw(key, shape, spread, most, cuts=(), kind=jnp.bfloat16):
    entries = spread * jax.random.normal(key, shape, jnp.float32)
    if cuts:
        entries = entries * block_scale(key, shape, cuts, -0.22, 0.18)
    return jnp.clip(entries, -most, most).astype(kind)


def setup_inputs(seed: int = 0) -> dict:
    streams_of = jax.random.split(jax.random.key(seed), 3)
    traces = bell_draw(streams_of[0], (NS, NR, NT), 1.0, 6.0, ((0, 16), (1, 8)))
    filters = bell_draw(streams_of[1], (NWIN, SPAN, TAPS), (SPAN * TAPS) ** -0.5, 0.25, (), jnp.float32)
    return {"traces": traces, "filters": filters}


def wave_table(freq_bins, sample_index):
    phases = freq_bins[:, None] * sample_index[None, :] % NT
    angles = phases.astype(jnp.float32) * jnp.float32(2.0 * math.pi / NT)
    return (jnp.cos(angles), jnp.sin(angles))

def complex_product(left_side, right_side):
    factor_product = partial(jnp.einsum, 'gjo,god->gjd', precision=lax.Precision.HIGHEST)
    part_real = factor_product(left_side[0], right_side[0]) - factor_product(left_side[1], right_side[1])
    part_imag = factor_product(left_side[0], right_side[1]) + factor_product(left_side[1], right_side[0])
    return jnp.stack([part_real, part_imag])

def response(filters, freq_bins):
    tap_index = jnp.arange(TAPS, dtype=jnp.int32)
    cosine_wave, sine_wave = wave_table(freq_bins, tap_index)
    filter_real = jnp.einsum('fk,wjk->fjw', cosine_wave, filters, precision=lax.Precision.HIGHEST)
    filter_imag = -jnp.einsum('fk,wjk->fjw', sine_wave, filters, precision=lax.Precision.HIGHEST)
    return (jnp.repeat(filter_real, RWIN, axis=2), jnp.repeat(filter_imag, RWIN, axis=2))

def apply_filter(extended, filter_real, filter_imag, source_count):
    sum_real = jnp.zeros(extended.shape[1:2] + (source_count,) + extended.shape[3:], jnp.float32)
    sum_imag = jnp.zeros_like(sum_real)
    for shifted in range(SPAN):
        part_real = extended[0, :, shifted:shifted + source_count, :]
        part_imag = extended[1, :, shifted:shifted + source_count, :]
        weight_real = filter_real[:, shifted][:, None, :]
        weight_imaginary = filter_imag[:, shifted][:, None, :]
        sum_real = sum_real + weight_real * part_real - weight_imaginary * part_imag
        sum_imag = sum_imag + weight_real * part_imag + weight_imaginary * part_real
    return jnp.stack([sum_real, sum_imag])

def reference(traces, filters):
    freq_bins = FLO + jnp.arange(NF, dtype=jnp.int32)
    cosine_wave, sine_wave = wave_table(freq_bins, jnp.arange(NT, dtype=jnp.int32))
    forward = (jnp.concatenate([cosine_wave, -sine_wave], 0) / jnp.float32(math.sqrt(NT))).astype(jnp.bfloat16)
    reciprocal_value = jnp.concatenate([cosine_wave, -sine_wave], 0).astype(jnp.bfloat16)
    flattened = traces.reshape(NS * NR, NT)
    spectra = jnp.dot(flattened, forward.T, preferred_element_type=jnp.float32).astype(jnp.bfloat16)
    spectrum = spectra.reshape(NS, NR, 2, NF).transpose(2, 3, 0, 1)
    widened = spectrum.astype(jnp.float32)
    order_one = (complex_product(widened, widened) / jnp.float32(math.sqrt(NS))).astype(jnp.bfloat16)
    order_two = complex_product(widened, order_one.astype(jnp.float32)) / jnp.float32(math.sqrt(NS))
    prediction = (order_one.astype(jnp.float32) - order_two).astype(jnp.bfloat16)
    rim_width = SPAN // 2
    extended = jnp.pad(prediction.astype(jnp.float32), ((0, 0), (0, 0), (rim_width, rim_width), (0, 0)))
    filter_real, filter_imag = response(filters, freq_bins)
    matched = apply_filter(extended, filter_real, filter_imag, NS).astype(jnp.bfloat16)
    matched_rows = matched.transpose(2, 3, 0, 1).reshape(NS * NR, 2 * NF)
    multiples = jnp.dot(matched_rows, reciprocal_value, preferred_element_type=jnp.float32) / jnp.float32(math.sqrt(NF))
    return (traces.astype(jnp.float32) - multiples.reshape(NS, NR, NT)).astype(jnp.bfloat16)
```

```python
import math

import jax
import jax.numpy as jnp
import numpy as np
from jax import lax
from jax.sharding import PartitionSpec as P

NS = 640
NT = 1024
NF = 96
FLO = 8
TAPS = 64
SPAN = 7
RWIN = 40
NWIN = 16
BOTH = ("freq", "panel")


def waves(freq_bins, samples):
    phases = np.outer(freq_bins, samples) % NT
    angles = phases.astype(np.float64) * (2.0 * math.pi / NT)
    return np.cos(angles), np.sin(angles)


def complex_product(left, right):
    def product(a, b):
        return jnp.dot(a, b, preferred_element_type=jnp.float32)

    real = product(left[0], right[0]) - product(left[1], right[1])
    imag = product(left[0], right[1]) + product(left[1], right[0])
    return jnp.stack([real, imag])


def solution(mesh):
    n_freq, n_panel = mesh.shape["freq"], mesh.shape["panel"]
    n_all = n_freq * n_panel
    bins = FLO + np.arange(NF)
    cosine, sine = waves(bins, np.arange(NT))
    table = np.stack([cosine, -sine], 1).reshape(2 * NF, NT)
    forward = (table / math.sqrt(NT)).astype(np.float32)
    inverse = table.astype(np.float32)
    tap_cos, tap_sin = waves(FLO + np.minimum(np.arange(n_all), NF - 1), np.arange(TAPS))
    taps = np.stack([tap_cos, -tap_sin], 1).astype(np.float32)
    rim = SPAN // 2

    def per_device(traces, filters):
        rows, cols, _ = traces.shape
        root = jnp.float32(math.sqrt(NS))
        flat = traces.reshape(rows * cols, NT)
        spectra = lax.dot_general(
            jnp.asarray(forward, jnp.bfloat16), flat, (((1,), (1,)), ((), ())),
            preferred_element_type=jnp.float32,
        ).astype(jnp.bfloat16)
        spectra = spectra.reshape(NF, 2, rows * cols)
        spectra = jnp.pad(spectra, ((0, n_all - NF), (0, 0), (0, 0)))
        slices = lax.all_to_all(spectra, BOTH, split_axis=0, concat_axis=0, tiled=True)
        slices = slices.reshape(n_freq, n_panel, 2, rows, cols)
        data = slices.transpose(2, 1, 3, 0, 4).reshape(2, NS, n_freq * cols)
        order_one = (complex_product(data, data) / root).astype(jnp.bfloat16)
        order_two = complex_product(data, order_one) / root
        prediction = (order_one.astype(jnp.float32) - order_two).astype(jnp.bfloat16)
        extended = jnp.pad(prediction, ((0, 0), (rim, rim), (0, 0))).astype(jnp.float32)
        me = lax.axis_index(BOTH)
        wave = lax.dynamic_index_in_dim(jnp.asarray(taps), me, 0, keepdims=False)
        reply = jnp.einsum("ck,wjk->cjw", wave, filters, precision=lax.Precision.HIGHEST)
        reply = jnp.repeat(reply, RWIN, axis=2)
        real = jnp.zeros((NS, n_freq * cols), jnp.float32)
        imag = real
        for j in range(SPAN):
            p_real, p_imag = extended[0, j : j + NS], extended[1, j : j + NS]
            real = real + reply[0, j] * p_real - reply[1, j] * p_imag
            imag = imag + reply[0, j] * p_imag + reply[1, j] * p_real
        matched = jnp.stack([real, imag]).astype(jnp.bfloat16)
        blocks = matched.reshape(2, n_panel, rows, n_freq, cols).transpose(3, 1, 0, 2, 4)
        blocks = blocks.reshape(n_all, 2, rows * cols)
        back = lax.all_to_all(blocks, BOTH, split_axis=0, concat_axis=0, tiled=True)
        back = back[:NF].reshape(2 * NF, rows * cols)
        multiples = lax.dot_general(
            back, jnp.asarray(inverse, jnp.bfloat16), (((0,), (0,)), ((), ())),
            preferred_element_type=jnp.float32,
        )
        multiples = multiples.reshape(rows, cols, NT) / jnp.float32(math.sqrt(NF))
        return (traces.astype(jnp.float32) - multiples).astype(jnp.bfloat16)

    placed = (P("panel", "freq", None), P())
    return jax.shard_map(
        per_device, mesh=mesh, in_specs=placed, out_specs=P("panel", "freq", None), check_vma=False
    )
```

```python
import functools
import math

import jax
import jax.numpy as jnp
import numpy as np
from jax import lax
from jax.experimental import pallas as pl
from jax.experimental.pallas import tpu as pltpu
from jax.sharding import PartitionSpec as P

NS = 640
NT = 1024
NF = 96
FLO = 8
TAPS = 64
SPAN = 7
RWIN = 40
NWIN = 16
BOTH = ("freq", "panel")


def waves(freq_bins, samples):
    phases = np.outer(freq_bins, samples) % NT
    angles = phases.astype(np.float64) * (2.0 * math.pi / NT)
    return np.cos(angles), np.sin(angles)


def mid_kernel(x_ref, w_ref, y_ref, z_ref, l_ref, r_ref, o_ref, f_ref, *, n_freq, n_panel, rows, cols):
    f32, bf16 = jnp.float32, jnp.bfloat16
    pair = 2 * n_panel
    width = n_freq * cols
    tiles = width // 128
    group = width // cols
    groups = rows // group
    lane = lax.broadcasted_iota(jnp.int32, (pair, 128), 1)
    root = 1.0 / math.sqrt(NS)

    def gather(read, outer, t):
        value = None
        for piece in range(group):
            lo, hi = max(piece * cols, t * 128), min((piece + 1) * cols, t * 128 + 128)
            if lo >= hi:
                continue
            src_lo = outer * cols + lo - piece * cols
            src_hi = src_lo + hi - lo
            for tile in range(src_lo // 128, (src_hi - 1) // 128 + 1):
                a, b = max(src_lo, tile * 128), min(src_hi, tile * 128 + 128)
                d0, d1 = a - src_lo + lo - t * 128, b - src_lo + lo - t * 128
                shift = (d0 - (a - tile * 128)) % 128
                v = read(piece, tile)
                if shift:
                    v = pltpu.roll(v, shift, 1)
                value = v if value is None else jnp.where((lane >= d0) & (lane < d1), v, value)
        return value

    def split(g, _):
        base = pl.multiple_of(g * width, 128)
        for s in range(group):
            def read(q, tile):
                return x_ref[q * pair:(q + 1) * pair, pl.ds(pl.multiple_of(base + tile * 128, 128), 128)].astype(f32)
            for t in range(tiles):
                z_ref[t, pl.ds(g * group + s, pair, stride=rows), :] = gather(read, s, t)
        return 0
    lax.fori_loop(0, groups, split, 0)

    def place(p, _):
        row = pl.multiple_of(p * 2 * rows, 16)
        for t in range(tiles):
            z = z_ref[t, pl.ds(pl.multiple_of(p * 4 * rows, 8), 4 * rows), :]
            re = jnp.concatenate([z[:rows], z[2 * rows:3 * rows]], 0)
            im = jnp.concatenate([z[rows:2 * rows], z[3 * rows:]], 0)
            c = slice(t * 128, t * 128 + 128); d = slice(width + t * 128, width + t * 128 + 128)
            reb, imb = re.astype(bf16), im.astype(bf16)
            l_ref[pl.ds(row, 2 * rows), c] = reb
            l_ref[pl.ds(row, 2 * rows), d] = imb
            r_ref[pl.ds(row, 2 * rows), c] = reb
            r_ref[pl.ds(row, 2 * rows), d] = imb
            r_ref[pl.ds(row + NS, 2 * rows), c] = (-im).astype(bf16)
            r_ref[pl.ds(row + NS, 2 * rows), d] = reb
        return 0
    lax.fori_loop(0, n_panel // 2, place, 0)

    step = 256
    for n in range(2 * width // step):
        c = slice(n * step, n * step + step)
        o = jnp.dot(l_ref[...], r_ref[:, c], preferred_element_type=f32) * root
        for h in range(step // 128):
            t = n * (step // 128) + h
            ob = o[:, h * 128:h * 128 + 128]
            o_ref[:NS, t * 128:t * 128 + 128] = ob.astype(bf16)
            if t < tiles:
                o_ref[NS:, width + t * 128:width + t * 128 + 128] = ob.astype(bf16)
            else:
                o_ref[NS:, (t - tiles) * 128:(t - tiles) * 128 + 128] = (-ob).astype(bf16)
    zero = jnp.zeros((8, 128), f32)
    for t in range(2 * tiles):
        f_ref[t, 0:8, :] = zero
        f_ref[t, 8 + NS:16 + NS, :] = zero
    for n in range(2 * width // step):
        c = slice(n * step, n * step + step)
        o = jnp.dot(l_ref[...], o_ref[:, c], preferred_element_type=f32) * root
        pred = (o_ref[:NS, c].astype(f32) - o).astype(bf16).astype(f32)
        for h in range(step // 128):
            f_ref[n * (step // 128) + h, 8:8 + NS, :] = pred[:, h * 128:h * 128 + 128]

    rim = SPAN // 2
    for t in range(tiles):
        weights = [jnp.broadcast_to(w_ref[i:i + 1, t * 128:t * 128 + 128], (rows, 128)) for i in range(2 * SPAN)]
        def match(p, _):
            real = imag = None
            for j in range(SPAN):
                at = pl.ds(p * rows + 8 - rim + j, rows)
                a, b = f_ref[t, at, :], f_ref[tiles + t, at, :]
                wr, wi = weights[j], weights[SPAN + j]
                re, im = wr * a - wi * b, wr * b + wi * a
                real, imag = (re, im) if real is None else (real + re, imag + im)
            z_ref[t, pl.ds(pl.multiple_of(p * 2 * rows, 8), rows), :] = real
            z_ref[t, pl.ds(pl.multiple_of(p * 2 * rows + rows, 8), rows), :] = imag
            return 0
        lax.fori_loop(0, n_panel, match, 0)

    def join(g, _):
        base = pl.multiple_of(g * width, 128)
        def read(s, tile):
            return z_ref[tile, pl.ds(g * group + s, pair, stride=rows), :]
        for q in range(n_freq):
            for t in range(tiles):
                y_ref[q * pair:(q + 1) * pair, pl.ds(pl.multiple_of(base + t * 128, 128), 128)] = gather(read, q, t).astype(bf16)
        return 0
    lax.fori_loop(0, groups, join, 0)


def middle(x, w, n_freq, n_panel, rows, cols):
    width = n_freq * cols
    f32, bf16 = jnp.float32, jnp.bfloat16
    return pl.pallas_call(
        functools.partial(mid_kernel, n_freq=n_freq, n_panel=n_panel, rows=rows, cols=cols),
        out_shape=jax.ShapeDtypeStruct(x.shape, bf16),
        scratch_shapes=[
            pltpu.VMEM((width // 128, 2 * NS, 128), f32),
            pltpu.VMEM((NS, 2 * width), bf16),
            pltpu.VMEM((2 * NS, 2 * width), bf16),
            pltpu.VMEM((2 * NS, 2 * width), bf16),
            pltpu.VMEM((2 * width // 128, NS + 16, 128), f32),
        ],
        compiler_params=pltpu.CompilerParams(vmem_limit_bytes=56 << 20),
    )(x, w)


def solution(mesh):
    n_freq, n_panel = mesh.shape["freq"], mesh.shape["panel"]
    n_all = n_freq * n_panel
    bins = FLO + np.arange(NF)
    cosine, sine = waves(bins, np.arange(NT))
    table = np.stack([cosine, -sine], 1).reshape(2 * NF, NT)
    forward = np.pad(table / math.sqrt(NT), ((0, 2 * (n_all - NF)), (0, 0))).astype(np.float32)
    inverse = table.astype(np.float32)
    tap_cos, tap_sin = waves(FLO + np.minimum(np.arange(n_all), NF - 1), np.arange(TAPS))
    taps = np.stack([tap_cos, -tap_sin], 1).astype(np.float32)

    def per_device(traces, filters):
        rows, cols, _ = traces.shape
        flat = traces.reshape(rows * cols, NT)
        spectra = lax.dot_general(
            jnp.asarray(forward, jnp.bfloat16), flat, (((1,), (1,)), ((), ())),
            preferred_element_type=jnp.float32,
        ).astype(jnp.bfloat16)
        spectra = spectra.reshape(n_all, 2, rows * cols)
        slices = lax.all_to_all(spectra, BOTH, split_axis=0, concat_axis=0, tiled=True)
        me = lax.axis_index(BOTH)
        wave = lax.dynamic_index_in_dim(jnp.asarray(taps), me, 0, keepdims=False)
        reply = jnp.einsum("ck,wjk->cjw", wave, filters, precision=lax.Precision.HIGHEST)
        reply = jnp.repeat(reply, RWIN, axis=2).reshape(2 * SPAN, n_freq * cols)
        matched = middle(
            slices.reshape(2 * n_all, rows * cols), reply, n_freq, n_panel, rows, cols
        ).reshape(n_all, 2, rows * cols)
        back = lax.all_to_all(matched, BOTH, split_axis=0, concat_axis=0, tiled=True)
        back = back[:NF].reshape(2 * NF, rows * cols)
        multiples = lax.dot_general(
            back, jnp.asarray(inverse, jnp.bfloat16), (((0,), (0,)), ((), ())),
            preferred_element_type=jnp.float32,
        )
        multiples = multiples.reshape(rows, cols, NT) / jnp.float32(math.sqrt(NF))
        return (traces.astype(jnp.float32) - multiples).astype(jnp.bfloat16)

    placed = (P("panel", "freq", None), P())
    return jax.shard_map(
        per_device, mesh=mesh, in_specs=placed, out_specs=P("panel", "freq", None), check_vma=False
    )
```

```python
import functools
import math

import jax
import jax.numpy as jnp
import numpy as np
from jax import lax
from jax.experimental import pallas as pl
from jax.experimental.pallas import tpu as pltpu
from jax.sharding import PartitionSpec as P

NS = 640
NT = 1024
NF = 96
FLO = 8
TAPS = 64
SPAN = 7
RWIN = 40
NWIN = 16
BOTH = ("freq", "panel")


def waves(freq_bins, samples):
    phases = np.outer(freq_bins, samples) % NT
    angles = phases.astype(np.float64) * (2.0 * math.pi / NT)
    return np.cos(angles), np.sin(angles)


def mid_kernel(x_ref, w_ref, y_ref, z_ref, l_ref, r_ref, o_ref, f_ref, *, n_freq, n_panel, rows, cols):
    f32, bf16 = jnp.float32, jnp.bfloat16
    pair = 2 * n_panel
    width = n_freq * cols
    tiles = width // 128
    group = width // cols
    groups = rows // group
    lane = lax.broadcasted_iota(jnp.int32, (pair, 128), 1)
    root = 1.0 / math.sqrt(NS)

    def gather(read, outer, t):
        value = None
        for piece in range(group):
            lo, hi = max(piece * cols, t * 128), min((piece + 1) * cols, t * 128 + 128)
            if lo >= hi:
                continue
            src_lo = outer * cols + lo - piece * cols
            src_hi = src_lo + hi - lo
            for tile in range(src_lo // 128, (src_hi - 1) // 128 + 1):
                a, b = max(src_lo, tile * 128), min(src_hi, tile * 128 + 128)
                d0, d1 = a - src_lo + lo - t * 128, b - src_lo + lo - t * 128
                shift = (d0 - (a - tile * 128)) % 128
                v = read(piece, tile)
                if shift:
                    v = pltpu.roll(v, shift, 1)
                value = v if value is None else jnp.where((lane >= d0) & (lane < d1), v, value)
        return value

    def split(g, _):
        base = pl.multiple_of(g * width, 128)
        for s in range(group):
            def read(q, tile):
                return x_ref[q * pair:(q + 1) * pair, pl.ds(pl.multiple_of(base + tile * 128, 128), 128)].astype(f32)
            for t in range(tiles):
                z_ref[t, pl.ds(g * group + s, pair, stride=rows), :] = gather(read, s, t)
        return 0
    lax.fori_loop(0, groups, split, 0)

    def place(p, _):
        row = pl.multiple_of(p * 2 * rows, 16)
        for t in range(tiles):
            z = z_ref[t, pl.ds(pl.multiple_of(p * 4 * rows, 8), 4 * rows), :]
            re = jnp.concatenate([z[:rows], z[2 * rows:3 * rows]], 0)
            im = jnp.concatenate([z[rows:2 * rows], z[3 * rows:]], 0)
            c = slice(t * 128, t * 128 + 128); d = slice(width + t * 128, width + t * 128 + 128)
            reb, imb = re.astype(bf16), im.astype(bf16)
            l_ref[pl.ds(row, 2 * rows), c] = reb
            l_ref[pl.ds(row, 2 * rows), d] = imb
            r_ref[pl.ds(row, 2 * rows), c] = reb
            r_ref[pl.ds(row, 2 * rows), d] = imb
            r_ref[pl.ds(row + NS, 2 * rows), c] = (-im).astype(bf16)
            r_ref[pl.ds(row + NS, 2 * rows), d] = reb
        return 0
    lax.fori_loop(0, n_panel // 2, place, 0)

    step = 256
    for n in range(2 * width // step):
        c = slice(n * step, n * step + step)
        o = jnp.dot(l_ref[...], r_ref[:, c], preferred_element_type=f32) * root
        for h in range(step // 128):
            t = n * (step // 128) + h
            ob = o[:, h * 128:h * 128 + 128]
            o_ref[:NS, t * 128:t * 128 + 128] = ob.astype(bf16)
            if t < tiles:
                o_ref[NS:, width + t * 128:width + t * 128 + 128] = ob.astype(bf16)
            else:
                o_ref[NS:, (t - tiles) * 128:(t - tiles) * 128 + 128] = (-ob).astype(bf16)
    zero = jnp.zeros((8, 128), f32)
    for t in range(2 * tiles):
        f_ref[t, 0:8, :] = zero
        f_ref[t, 8 + NS:16 + NS, :] = zero
    for n in range(2 * width // step):
        c = slice(n * step, n * step + step)
        o = jnp.dot(l_ref[...], o_ref[:, c], preferred_element_type=f32) * root
        pred = (o_ref[:NS, c].astype(f32) - o).astype(bf16).astype(f32)
        for h in range(step // 128):
            f_ref[n * (step // 128) + h, 8:8 + NS, :] = pred[:, h * 128:h * 128 + 128]

    rim = SPAN // 2
    for t in range(tiles):
        weights = [jnp.broadcast_to(w_ref[i:i + 1, t * 128:t * 128 + 128], (rows, 128)) for i in range(2 * SPAN)]
        def match(p, _):
            real = imag = None
            for j in range(SPAN):
                at = pl.ds(p * rows + 8 - rim + j, rows)
                a, b = f_ref[t, at, :], f_ref[tiles + t, at, :]
                wr, wi = weights[j], weights[SPAN + j]
                re, im = wr * a - wi * b, wr * b + wi * a
                real, imag = (re, im) if real is None else (real + re, imag + im)
            z_ref[t, pl.ds(pl.multiple_of(p * 2 * rows, 8), rows), :] = real
            z_ref[t, pl.ds(pl.multiple_of(p * 2 * rows + rows, 8), rows), :] = imag
            return 0
        lax.fori_loop(0, n_panel, match, 0)

    def join(g, _):
        base = pl.multiple_of(g * width, 128)
        def read(s, tile):
            return z_ref[tile, pl.ds(g * group + s, pair, stride=rows), :]
        for q in range(n_freq):
            for t in range(tiles):
                y_ref[q * pair:(q + 1) * pair, pl.ds(pl.multiple_of(base + t * 128, 128), 128)] = gather(read, q, t).astype(bf16)
        return 0
    lax.fori_loop(0, groups, join, 0)


def middle(x, w, n_freq, n_panel, rows, cols):
    width = n_freq * cols
    f32, bf16 = jnp.float32, jnp.bfloat16
    return pl.pallas_call(
        functools.partial(mid_kernel, n_freq=n_freq, n_panel=n_panel, rows=rows, cols=cols),
        out_shape=pltpu.VMEM(x.shape, bf16),
        in_specs=[pl.BlockSpec(memory_space=pltpu.VMEM)] * 2,
        out_specs=pl.BlockSpec(memory_space=pltpu.VMEM),
        scratch_shapes=[
            pltpu.VMEM((width // 128, 2 * NS, 128), f32),
            pltpu.VMEM((NS, 2 * width), bf16),
            pltpu.VMEM((2 * NS, 2 * width), bf16),
            pltpu.VMEM((2 * NS, 2 * width), bf16),
            pltpu.VMEM((2 * width // 128, NS + 16, 128), f32),
        ],
        compiler_params=pltpu.CompilerParams(vmem_limit_bytes=22 << 20),
    )(x, w)


def first_kernel(t_hbm, f_ref, s_ref, t_ref, sem, *, group):
    rows, cols, _ = t_ref.shape
    width, half = group * cols, group * cols // 2
    used = f_ref.shape[1]

    def copy(g):
        at = pl.ds(g * group, group)
        return pltpu.make_async_copy(t_hbm.at[at], t_ref.at[at], sem.at[g])

    for g in range(rows // group):
        copy(g).start()
    s_ref[used:, :] = jnp.zeros((s_ref.shape[0] - used, s_ref.shape[1]), s_ref.dtype)
    for g in range(rows // group):
        copy(g).wait()
        block = t_ref[g * group : (g + 1) * group].reshape(width, NT)
        out = jnp.concatenate(
            [
                jnp.dot(part, f_ref[...], preferred_element_type=jnp.float32)
                for part in (block[:half], block[half:])
            ],
            0,
        )
        s_ref[:used, g * width : (g + 1) * width] = out.astype(s_ref.dtype).T


def first(traces, forward, n_all, group=8):
    rows, cols, _ = traces.shape
    return pl.pallas_call(
        functools.partial(first_kernel, group=group),
        out_shape=pltpu.VMEM((2 * n_all, rows * cols), jnp.bfloat16),
        in_specs=[
            pl.BlockSpec(memory_space=pltpu.HBM),
            pl.BlockSpec(memory_space=pltpu.VMEM),
        ],
        out_specs=pl.BlockSpec(memory_space=pltpu.VMEM),
        scratch_shapes=[pltpu.VMEM(traces.shape, jnp.bfloat16), pltpu.SemaphoreType.DMA((rows // group,))],
        compiler_params=pltpu.CompilerParams(vmem_limit_bytes=20 << 20),
    )(pltpu.with_memory_space_constraint(traces, pltpu.HBM), forward)


def last_kernel(m_ref, t_hbm, i_ref, o_hbm, t_ref, o_ref, t_sem, sem, *, group, part):
    rows, cols, _ = t_ref.shape
    width = group * cols
    used = i_ref.shape[0]
    scale = 1.0 / math.sqrt(NF)
    steps = group // part
    def copy(g, h):
        at = pl.ds(g * group + h * part, part)
        return pltpu.make_async_copy(o_ref.at[at], o_hbm.at[at], sem)
    def fetch(g):
        at = pl.ds(g * group, group)
        return pltpu.make_async_copy(t_hbm.at[at], t_ref.at[at], t_sem.at[g])

    for g in range(rows // group):
        fetch(g).start()
    for g in range(rows // group):
        fetch(g).wait()
        mt = m_ref[:used, g * width:(g + 1) * width].T
        for h in range(steps):
            acc = jnp.dot(mt[h * part * cols:(h + 1) * part * cols], i_ref[...], preferred_element_type=jnp.float32)
            at = slice(g * group + h * part, g * group + (h + 1) * part)
            t = t_ref[at].astype(jnp.float32)
            o_ref[at] = (t - (acc * scale).reshape(t.shape)).astype(o_ref.dtype)
            copy(g, h).start()
    pltpu.make_async_copy(o_ref, o_hbm, sem).wait()


def last(m, traces, inverse, group=8, part=2):
    return pl.pallas_call(
        functools.partial(last_kernel, group=group, part=part),
        out_shape=jax.ShapeDtypeStruct(traces.shape, jnp.bfloat16),
        in_specs=[
            pl.BlockSpec(memory_space=pltpu.VMEM),
            pl.BlockSpec(memory_space=pltpu.HBM),
            pl.BlockSpec(memory_space=pltpu.VMEM),
        ],
        out_specs=pl.BlockSpec(memory_space=pltpu.HBM),
        scratch_shapes=[
            pltpu.VMEM(traces.shape, jnp.bfloat16),
            pltpu.VMEM(traces.shape, jnp.bfloat16),
            pltpu.SemaphoreType.DMA((traces.shape[0] // group,)),
            pltpu.SemaphoreType.DMA(()),
        ],
        compiler_params=pltpu.CompilerParams(vmem_limit_bytes=24 << 20),
    )(m, pltpu.with_memory_space_constraint(traces, pltpu.HBM), inverse)


def solution(mesh):
    n_freq, n_panel = mesh.shape["freq"], mesh.shape["panel"]
    n_all = n_freq * n_panel
    bins = FLO + np.arange(NF)
    cosine, sine = waves(bins, np.arange(NT))
    table = np.stack([cosine, -sine], 1).reshape(2 * NF, NT)
    forward = (table / math.sqrt(NT)).astype(np.float32).T
    inverse = table.astype(np.float32)
    tap_cos, tap_sin = waves(FLO + np.minimum(np.arange(n_all), NF - 1), np.arange(TAPS))
    taps = np.stack([tap_cos, -tap_sin], 1).astype(np.float32)

    def per_device(traces, filters):
        rows, cols, _ = traces.shape
        spectra = first(traces, jnp.asarray(forward, jnp.bfloat16), n_all)
        spectra = spectra.reshape(n_all, 2, rows * cols)
        slices = lax.all_to_all(spectra, BOTH, split_axis=0, concat_axis=0, tiled=True)
        me = lax.axis_index(BOTH)
        wave = lax.dynamic_index_in_dim(jnp.asarray(taps), me, 0, keepdims=False)
        reply = jnp.einsum("ck,wjk->cjw", wave, filters, precision=lax.Precision.HIGHEST)
        reply = jnp.repeat(reply, RWIN, axis=2).reshape(2 * SPAN, n_freq * cols)
        matched = middle(
            slices.reshape(2 * n_all, rows * cols), reply, n_freq, n_panel, rows, cols
        ).reshape(n_all, 2, rows * cols)
        back = lax.all_to_all(matched, BOTH, split_axis=0, concat_axis=0, tiled=True)
        back = back.reshape(2 * n_all, rows * cols)
        return last(back, traces, jnp.asarray(inverse, jnp.bfloat16))

    placed = (P("panel", "freq", None), P())
    return jax.shard_map(
        per_device, mesh=mesh, in_specs=placed, out_specs=P("panel", "freq", None), check_vma=False
    )
```

```python
import functools
import math

import jax
import jax.numpy as jnp
import numpy as np
from jax import lax
from jax.experimental import pallas as pl
from jax.experimental.pallas import tpu as pltpu
from jax.sharding import PartitionSpec as P

NS = 640
NT = 1024
NF = 96
FLO = 8
TAPS = 64
SPAN = 7
RWIN = 40
NWIN = 16
BOTH = ("freq", "panel")


def waves(freq_bins, samples):
    phases = np.outer(freq_bins, samples) % NT
    angles = phases.astype(np.float64) * (2.0 * math.pi / NT)
    return np.cos(angles), np.sin(angles)


def mid_kernel(x_ref, w_ref, y_ref, z_ref, l_ref, r_ref, o_ref, f_ref, *, n_freq, n_panel, rows, cols):
    f32, bf16 = jnp.float32, jnp.bfloat16
    pair = 2 * n_panel
    width = n_freq * cols
    tiles = width // 128
    group = width // cols
    groups = rows // group
    lane = lax.broadcasted_iota(jnp.int32, (pair, 128), 1)
    root = 1.0 / math.sqrt(NS)

    def gather(read, outer, t):
        value = None
        for piece in range(group):
            lo, hi = max(piece * cols, t * 128), min((piece + 1) * cols, t * 128 + 128)
            if lo >= hi:
                continue
            src_lo = outer * cols + lo - piece * cols
            src_hi = src_lo + hi - lo
            for tile in range(src_lo // 128, (src_hi - 1) // 128 + 1):
                a, b = max(src_lo, tile * 128), min(src_hi, tile * 128 + 128)
                d0, d1 = a - src_lo + lo - t * 128, b - src_lo + lo - t * 128
                shift = (d0 - (a - tile * 128)) % 128
                v = read(piece, tile)
                if shift:
                    v = pltpu.roll(v, shift, 1)
                value = v if value is None else jnp.where((lane >= d0) & (lane < d1), v, value)
        return value

    def split(g, _):
        base = pl.multiple_of(g * width, 128)
        for s in range(group):
            def read(q, tile):
                lanes = pl.ds(pl.multiple_of(base + tile * 128, 128), 128)
                return x_ref[q * n_panel:(q + 1) * n_panel, :, lanes].reshape(pair, 128).astype(f32)
            for t in range(tiles):
                z_ref[t, pl.ds(g * group + s, pair, stride=rows), :] = gather(read, s, t)
        return 0
    lax.fori_loop(0, groups, split, 0)

    def place(p, _):
        row = pl.multiple_of(p * 2 * rows, 16)
        for t in range(tiles):
            z = z_ref[t, pl.ds(pl.multiple_of(p * 4 * rows, 8), 4 * rows), :]
            re = jnp.concatenate([z[:rows], z[2 * rows:3 * rows]], 0)
            im = jnp.concatenate([z[rows:2 * rows], z[3 * rows:]], 0)
            c = slice(t * 128, t * 128 + 128); d = slice(width + t * 128, width + t * 128 + 128)
            reb, imb = re.astype(bf16), im.astype(bf16)
            l_ref[pl.ds(row, 2 * rows), c] = reb
            l_ref[pl.ds(row, 2 * rows), d] = imb
            r_ref[pl.ds(row, 2 * rows), c] = reb
            r_ref[pl.ds(row, 2 * rows), d] = imb
            r_ref[pl.ds(row + NS, 2 * rows), c] = (-im).astype(bf16)
            r_ref[pl.ds(row + NS, 2 * rows), d] = reb
        return 0
    lax.fori_loop(0, n_panel // 2, place, 0)

    step = 256
    for n in range(2 * width // step):
        c = slice(n * step, n * step + step)
        o = jnp.dot(l_ref[...], r_ref[:, c], preferred_element_type=f32) * root
        for h in range(step // 128):
            t = n * (step // 128) + h
            ob = o[:, h * 128:h * 128 + 128]
            o_ref[:NS, t * 128:t * 128 + 128] = ob.astype(bf16)
            if t < tiles:
                o_ref[NS:, width + t * 128:width + t * 128 + 128] = ob.astype(bf16)
            else:
                o_ref[NS:, (t - tiles) * 128:(t - tiles) * 128 + 128] = (-ob).astype(bf16)
    zero = jnp.zeros((8, 128), f32)
    for t in range(3 * tiles):
        f_ref[t, 0:8, :] = zero
        f_ref[t, 8 + NS:16 + NS, :] = zero
    for n in range(2 * width // step):
        c = slice(n * step, n * step + step)
        o = jnp.dot(l_ref[...], o_ref[:, c], preferred_element_type=f32) * root
        pred = (o_ref[:NS, c].astype(f32) - o).astype(bf16).astype(f32)
        for h in range(step // 128):
            t = n * (step // 128) + h
            f_ref[t, 8:8 + NS, :] = pred[:, h * 128:h * 128 + 128]
            if t >= tiles:
                f_ref[t + tiles, 8:8 + NS, :] = f_ref[t - tiles, 8:8 + NS, :] + pred[:, h * 128:h * 128 + 128]

    rim = SPAN // 2
    for t in range(tiles):
        weights = [jnp.broadcast_to(w_ref[i:i + 1, t * 128:t * 128 + 128], (rows, 128)) for i in range(3 * SPAN)]

        def match(p, _):
            sums = [None] * 3
            for j in range(SPAN):
                at = pl.ds(p * rows + 8 - rim + j, rows)
                for i, plane in enumerate((2 * tiles + t, tiles + t, t)):
                    term = weights[i * SPAN + j] * f_ref[plane, at, :]
                    sums[i] = term if sums[i] is None else sums[i] + term
            z_ref[t, pl.ds(pl.multiple_of(p * 2 * rows, 8), rows), :] = sums[0] - sums[1]
            z_ref[t, pl.ds(pl.multiple_of(p * 2 * rows + rows, 8), rows), :] = sums[0] + sums[2]
            return 0

        lax.fori_loop(0, n_panel, match, 0)

    def join(g, _):
        base = pl.multiple_of(g * width, 128)
        def read(s, tile):
            return z_ref[tile, pl.ds(g * group + s, pair, stride=rows), :]
        for q in range(n_freq):
            for t in range(tiles):
                lanes = pl.ds(pl.multiple_of(base + t * 128, 128), 128)
                y_ref[q * n_panel:(q + 1) * n_panel, :, lanes] = gather(read, q, t).astype(bf16).reshape(n_panel, 2, 128)
        return 0
    lax.fori_loop(0, groups, join, 0)


def middle(x, w, n_freq, n_panel, rows, cols):
    width = n_freq * cols
    f32, bf16 = jnp.float32, jnp.bfloat16
    return pl.pallas_call(
        functools.partial(mid_kernel, n_freq=n_freq, n_panel=n_panel, rows=rows, cols=cols),
        out_shape=pltpu.VMEM(x.shape, bf16),
        in_specs=[pl.BlockSpec(memory_space=pltpu.VMEM)] * 2,
        out_specs=pl.BlockSpec(memory_space=pltpu.VMEM),
        scratch_shapes=[
            pltpu.VMEM((width // 128, 2 * NS, 128), f32),
            pltpu.VMEM((NS, 2 * width), bf16),
            pltpu.VMEM((2 * NS, 2 * width), bf16),
            pltpu.VMEM((2 * NS, 2 * width), bf16),
            pltpu.VMEM((3 * width // 128, NS + 16, 128), f32),
        ],
        compiler_params=pltpu.CompilerParams(vmem_limit_bytes=22 << 20),
    )(
        pltpu.with_memory_space_constraint(x, pltpu.VMEM),
        pltpu.with_memory_space_constraint(w, pltpu.VMEM),
    )


def first_kernel(t_hbm, f_hbm, tap_hbm, filt_hbm, s_ref, t_ref, w_ref, f_ref, tap_ref, filt_ref, sem, *, group):
    rows, cols, _ = t_ref.shape
    width, half = group * cols, group * cols // 2
    used = f_ref.shape[1] // 2

    def fetch(g):
        at = pl.ds(g * group, group)
        return pltpu.make_async_copy(t_hbm.at[at], t_ref.at[at], sem.at[g])

    table = pltpu.make_async_copy(f_hbm, f_ref, sem.at[rows // group])
    tap = pltpu.make_async_copy(tap_hbm.at[lax.axis_index(BOTH)], tap_ref, sem.at[rows // group + 1])
    filt = pltpu.make_async_copy(filt_hbm, filt_ref, sem.at[rows // group + 2])
    tap.start()
    filt.start()
    table.start()
    for g in range(rows // group):
        fetch(g).start()
    s_ref[used:] = jnp.zeros((s_ref.shape[0] - used,) + s_ref.shape[1:], s_ref.dtype)
    tap.wait()
    filt.wait()
    window = lax.broadcasted_iota(jnp.int32, (NWIN, w_ref.shape[1]), 0) * RWIN
    place = lax.broadcasted_iota(jnp.int32, (NWIN, w_ref.shape[1]), 1) - window
    inside = (place >= 0) & (place < RWIN)
    for j in range(SPAN):
        real, imag = (
            jnp.sum(
                jnp.where(inside, jnp.sum(filt_ref[j] * tap_ref[c : c + 1, :], 1, keepdims=True), 0.0),
                0,
                keepdims=True,
            )
            for c in range(2)
        )
        w_ref[j : j + 1, :] = real
        w_ref[SPAN + j : SPAN + j + 1, :] = real + imag
        w_ref[2 * SPAN + j : 2 * SPAN + j + 1, :] = imag - real
    table.wait()
    for g in range(rows // group):
        fetch(g).wait()
        block = t_ref[g * group : (g + 1) * group].reshape(width, NT)
        out = jnp.concatenate(
            [
                jnp.dot(part, f_ref[...], preferred_element_type=jnp.float32)
                for part in (block[:half], block[half:])
            ],
            0,
        )
        s_ref[:used, :, g * width : (g + 1) * width] = out.astype(s_ref.dtype).T.reshape(used, 2, width)


def first(traces, forward, taps, filters, n_all, receivers, group=8):
    rows, cols, _ = traces.shape
    hbm, vmem = pl.BlockSpec(memory_space=pltpu.HBM), pl.BlockSpec(memory_space=pltpu.VMEM)
    return pl.pallas_call(
        functools.partial(first_kernel, group=group),
        out_shape=(
            pltpu.VMEM((n_all, 2, rows * cols), jnp.bfloat16),
            pltpu.VMEM(traces.shape, jnp.bfloat16),
            pltpu.VMEM((3 * SPAN, receivers), jnp.float32),
        ),
        in_specs=[hbm] * 4,
        out_specs=(vmem, vmem, vmem),
        scratch_shapes=[
            pltpu.VMEM(forward.shape, jnp.bfloat16),
            pltpu.VMEM(taps.shape[1:], jnp.float32),
            pltpu.VMEM(filters.shape, jnp.float32),
            pltpu.SemaphoreType.DMA((rows // group + 3,)),
        ],
        compiler_params=pltpu.CompilerParams(vmem_limit_bytes=12 << 20),
    )(
        pltpu.with_memory_space_constraint(traces, pltpu.HBM),
        pltpu.with_memory_space_constraint(forward, pltpu.HBM),
        pltpu.with_memory_space_constraint(taps, pltpu.HBM),
        pltpu.with_memory_space_constraint(filters, pltpu.HBM),
    )


def last_kernel(m_ref, t_ref, i_ref, o_hbm, o_ref, sem, *, group, part):
    rows, cols, _ = t_ref.shape
    width = group * cols
    used = i_ref.shape[0]
    scale = 1.0 / math.sqrt(NF)

    def send(at):
        return pltpu.make_async_copy(o_ref.at[at], o_hbm.at[at], sem)

    for g in range(rows // group):
        m = m_ref[: used // 2, :, g * width : (g + 1) * width].reshape(used, width).T
        for h in range(group // part):
            acc = jnp.dot(
                m[h * part * cols : (h + 1) * part * cols], i_ref[...], preferred_element_type=jnp.float32
            )
            at = pl.ds(g * group + h * part, part)
            t = t_ref[at].astype(jnp.float32)
            o_ref[at] = (t - (acc * scale).reshape(t.shape)).astype(o_ref.dtype)
            send(at).start()
    pltpu.make_async_copy(o_ref, o_hbm, sem).wait()


def last(m, traces, inverse, group=8, part=2):
    vmem = pl.BlockSpec(memory_space=pltpu.VMEM)
    return pl.pallas_call(
        functools.partial(last_kernel, group=group, part=part),
        out_shape=jax.ShapeDtypeStruct(traces.shape, jnp.bfloat16),
        in_specs=[vmem, vmem, vmem],
        out_specs=pl.BlockSpec(memory_space=pltpu.HBM),
        scratch_shapes=[
            pltpu.VMEM(traces.shape, jnp.bfloat16),
            pltpu.SemaphoreType.DMA(()),
        ],
        compiler_params=pltpu.CompilerParams(vmem_limit_bytes=16 << 20),
    )(
        pltpu.with_memory_space_constraint(m, pltpu.VMEM),
        pltpu.with_memory_space_constraint(traces, pltpu.VMEM),
        inverse,
    )


def solution(mesh):
    n_freq, n_panel = mesh.shape["freq"], mesh.shape["panel"]
    n_all = n_freq * n_panel
    bins = FLO + np.arange(NF)
    cosine, sine = waves(bins, np.arange(NT))
    table = np.stack([cosine, -sine], 1).reshape(2 * NF, NT)
    forward = (table / math.sqrt(NT)).astype(np.float32).T
    inverse = table.astype(np.float32)
    tap_cos, tap_sin = waves(FLO + np.minimum(np.arange(n_all), NF - 1), np.arange(TAPS))
    taps = np.stack([tap_cos, -tap_sin], 1).astype(np.float32)

    def per_device(traces, filters):
        rows, cols, _ = traces.shape
        spectra, kept, reply = first(
            traces,
            jnp.asarray(forward, jnp.bfloat16),
            jnp.asarray(taps),
            filters.transpose(1, 0, 2),
            n_all,
            n_freq * cols,
        )
        slices = lax.all_to_all(spectra, BOTH, split_axis=0, concat_axis=0, tiled=True)
        matched = middle(slices, reply, n_freq, n_panel, rows, cols)
        back = lax.all_to_all(matched, BOTH, split_axis=0, concat_axis=0, tiled=True)
        return last(back, kept, jnp.asarray(inverse, jnp.bfloat16))

    placed = (P("panel", "freq", None), P())
    return jax.shard_map(
        per_device, mesh=mesh, in_specs=placed, out_specs=P("panel", "freq", None), check_vma=False
    )
```

```python
import functools
import math

import jax
import jax.numpy as jnp
import numpy as np
from jax import lax
from jax.experimental import pallas as pl
from jax.experimental.pallas import tpu as pltpu
from jax.sharding import PartitionSpec as P

NS = 640
NT = 1024
NF = 96
FLO = 8
TAPS = 64
SPAN = 7
RWIN = 40
NWIN = 16
BOTH = ("freq", "panel")


def waves(freq_bins, samples):
    phases = np.outer(freq_bins, samples) % NT
    angles = phases.astype(np.float64) * (2.0 * math.pi / NT)
    return np.cos(angles), np.sin(angles)


def mid_kernel(x_ref, w_ref, y_ref, z_ref, l_ref, r_ref, o_ref, f_ref, xs_ref, *, n_freq, n_panel, rows, cols):
    f32, bf16 = jnp.float32, jnp.bfloat16
    pair = 2 * n_panel
    width = n_freq * cols
    tiles = width // 128
    group = width // cols
    groups = rows // group
    lane = lax.broadcasted_iota(jnp.int32, (pair, 128), 1)
    root = 1.0 / math.sqrt(NS)

    def gather(read, outer, t):
        value = None
        for piece in range(group):
            lo, hi = max(piece * cols, t * 128), min((piece + 1) * cols, t * 128 + 128)
            if lo >= hi:
                continue
            src_lo = outer * cols + lo - piece * cols
            src_hi = src_lo + hi - lo
            for tile in range(src_lo // 128, (src_hi - 1) // 128 + 1):
                a, b = max(src_lo, tile * 128), min(src_hi, tile * 128 + 128)
                d0, d1 = a - src_lo + lo - t * 128, b - src_lo + lo - t * 128
                shift = (d0 - (a - tile * 128)) % 128
                v = read(piece, tile)
                if shift:
                    v = pltpu.roll(v, shift, 1)
                value = v if value is None else jnp.where((lane >= d0) & (lane < d1), v, value)
        return value

    for q in range(n_freq):
        xs_ref[q * pair:(q + 1) * pair] = x_ref[q * n_panel:(q + 1) * n_panel].reshape(pair, rows * cols)

    def split(g, _):
        base = pl.multiple_of(g * width, 128)
        for s in range(group):
            def read(q, tile):
                return xs_ref[q * pair:(q + 1) * pair, pl.ds(pl.multiple_of(base + tile * 128, 128), 128)]
            for t in range(tiles):
                z_ref[t, pl.ds(g * group + s, pair, stride=rows), :] = gather(read, s, t).astype(f32)
        return 0
    lax.fori_loop(0, groups, split, 0)

    def place(p, _):
        row = pl.multiple_of(p * 2 * rows, 16)
        for t in range(tiles):
            z = z_ref[t, pl.ds(pl.multiple_of(p * 4 * rows, 8), 4 * rows), :]
            re = jnp.concatenate([z[:rows], z[2 * rows:3 * rows]], 0)
            im = jnp.concatenate([z[rows:2 * rows], z[3 * rows:]], 0)
            c = slice(t * 128, t * 128 + 128); d = slice(width + t * 128, width + t * 128 + 128)
            reb, imb = re.astype(bf16), im.astype(bf16)
            l_ref[pl.ds(row, 2 * rows), c] = reb
            l_ref[pl.ds(row, 2 * rows), d] = imb
            r_ref[pl.ds(row, 2 * rows), c] = reb
            r_ref[pl.ds(row, 2 * rows), d] = imb
            r_ref[pl.ds(row + NS, 2 * rows), c] = (-im).astype(bf16)
            r_ref[pl.ds(row + NS, 2 * rows), d] = reb
        return 0
    lax.fori_loop(0, n_panel // 2, place, 0)

    step = 256
    for n in range(2 * width // step):
        c = slice(n * step, n * step + step)
        o = jnp.dot(l_ref[...], r_ref[:, c], preferred_element_type=f32) * root
        for h in range(step // 128):
            t = n * (step // 128) + h
            ob = o[:, h * 128:h * 128 + 128]
            o_ref[:NS, t * 128:t * 128 + 128] = ob.astype(bf16)
            if t < tiles:
                o_ref[NS:, width + t * 128:width + t * 128 + 128] = ob.astype(bf16)
            else:
                o_ref[NS:, (t - tiles) * 128:(t - tiles) * 128 + 128] = (-ob).astype(bf16)
    zero = jnp.zeros((8, 128), f32)
    for t in range(3 * tiles):
        f_ref[t, 0:8, :] = zero
        f_ref[t, 8 + NS:16 + NS, :] = zero
    for n in range(2 * width // step):
        c = slice(n * step, n * step + step)
        o = jnp.dot(l_ref[...], o_ref[:, c], preferred_element_type=f32) * root
        pred = (o_ref[:NS, c].astype(f32) - o).astype(bf16).astype(f32)
        for h in range(step // 128):
            t = n * (step // 128) + h
            f_ref[t, 8:8 + NS, :] = pred[:, h * 128:h * 128 + 128]
            if t >= tiles:
                f_ref[t + tiles, 8:8 + NS, :] = f_ref[t - tiles, 8:8 + NS, :] + pred[:, h * 128:h * 128 + 128]

    rim = SPAN // 2
    for t in range(tiles):
        weights = [jnp.broadcast_to(w_ref[i:i + 1, t * 128:t * 128 + 128], (rows, 128)) for i in range(3 * SPAN)]

        def match(p, _):
            sums = [None] * 3
            for j in range(SPAN):
                at = pl.ds(p * rows + 8 - rim + j, rows)
                for i, plane in enumerate((2 * tiles + t, tiles + t, t)):
                    term = weights[i * SPAN + j] * f_ref[plane, at, :]
                    sums[i] = term if sums[i] is None else sums[i] + term
            z_ref[t, pl.ds(pl.multiple_of(p * 2 * rows, 8), rows), :] = sums[0] - sums[1]
            z_ref[t, pl.ds(pl.multiple_of(p * 2 * rows + rows, 8), rows), :] = sums[0] + sums[2]
            return 0

        lax.fori_loop(0, n_panel, match, 0, unroll=4)

    def join(g, _):
        base = pl.multiple_of(g * width, 128)
        def read(s, tile):
            return z_ref[tile, pl.ds(g * group + s, pair, stride=rows), :].astype(bf16)
        for q in range(n_freq):
            for t in range(tiles):
                xs_ref[q * pair:(q + 1) * pair, pl.ds(pl.multiple_of(base + t * 128, 128), 128)] = gather(read, q, t)
        return 0
    lax.fori_loop(0, groups, join, 0)
    for q in range(n_freq):
        y_ref[q * n_panel:(q + 1) * n_panel] = xs_ref[q * pair:(q + 1) * pair].reshape(n_panel, 2, rows * cols)


def middle(x, w, n_freq, n_panel, rows, cols):
    width = n_freq * cols
    f32, bf16 = jnp.float32, jnp.bfloat16
    return pl.pallas_call(
        functools.partial(mid_kernel, n_freq=n_freq, n_panel=n_panel, rows=rows, cols=cols),
        out_shape=pltpu.VMEM(x.shape, bf16),
        in_specs=[pl.BlockSpec(memory_space=pltpu.VMEM)] * 2,
        out_specs=pl.BlockSpec(memory_space=pltpu.VMEM),
        scratch_shapes=[
            pltpu.VMEM((width // 128, 2 * NS, 128), f32),
            pltpu.VMEM((NS, 2 * width), bf16),
            pltpu.VMEM((2 * NS, 2 * width), bf16),
            pltpu.VMEM((2 * NS, 2 * width), bf16),
            pltpu.VMEM((3 * width // 128, NS + 16, 128), f32),
            pltpu.VMEM((2 * n_freq * n_panel, rows * cols), bf16),
        ],
        compiler_params=pltpu.CompilerParams(vmem_limit_bytes=26 << 20),
    )(
        pltpu.with_memory_space_constraint(x, pltpu.VMEM),
        pltpu.with_memory_space_constraint(w, pltpu.VMEM),
    )


def first_kernel(t_hbm, f_hbm, tap_hbm, filt_hbm, s_ref, t_ref, w_ref, f_ref, tap_ref, filt_ref, sem, *, group):
    rows, cols, _ = t_ref.shape
    width, half = group * cols, group * cols // 2
    used = f_ref.shape[1] // 2

    def fetch(g):
        at = pl.ds(g * group, group)
        return pltpu.make_async_copy(t_hbm.at[at], t_ref.at[at], sem.at[g])

    table = pltpu.make_async_copy(f_hbm, f_ref, sem.at[rows // group])
    tap = pltpu.make_async_copy(tap_hbm.at[lax.axis_index(BOTH)], tap_ref, sem.at[rows // group + 1])
    filt = pltpu.make_async_copy(filt_hbm, filt_ref, sem.at[rows // group + 2])
    tap.start()
    filt.start()
    table.start()
    for g in range(rows // group):
        fetch(g).start()
    s_ref[used:] = jnp.zeros((s_ref.shape[0] - used,) + s_ref.shape[1:], s_ref.dtype)
    tap.wait()
    filt.wait()
    window = lax.broadcasted_iota(jnp.int32, (NWIN, w_ref.shape[1]), 0) * RWIN
    place = lax.broadcasted_iota(jnp.int32, (NWIN, w_ref.shape[1]), 1) - window
    inside = (place >= 0) & (place < RWIN)
    for j in range(SPAN):
        real, imag = (
            jnp.sum(
                jnp.where(inside, jnp.sum(filt_ref[j] * tap_ref[c : c + 1, :], 1, keepdims=True), 0.0),
                0,
                keepdims=True,
            )
            for c in range(2)
        )
        w_ref[j : j + 1, :] = real
        w_ref[SPAN + j : SPAN + j + 1, :] = real + imag
        w_ref[2 * SPAN + j : 2 * SPAN + j + 1, :] = imag - real
    table.wait()
    for g in range(rows // group):
        fetch(g).wait()
        block = t_ref[g * group : (g + 1) * group].reshape(width, NT)
        out = jnp.concatenate(
            [
                jnp.dot(part, f_ref[...], preferred_element_type=jnp.float32)
                for part in (block[:half], block[half:])
            ],
            0,
        )
        s_ref[:used, :, g * width : (g + 1) * width] = out.astype(s_ref.dtype).T.reshape(used, 2, width)


def first(traces, forward, taps, filters, n_all, receivers, group=8):
    rows, cols, _ = traces.shape
    hbm, vmem = pl.BlockSpec(memory_space=pltpu.HBM), pl.BlockSpec(memory_space=pltpu.VMEM)
    return pl.pallas_call(
        functools.partial(first_kernel, group=group),
        out_shape=(
            pltpu.VMEM((n_all, 2, rows * cols), jnp.bfloat16),
            pltpu.VMEM(traces.shape, jnp.bfloat16),
            pltpu.VMEM((3 * SPAN, receivers), jnp.float32),
        ),
        in_specs=[hbm] * 4,
        out_specs=(vmem, vmem, vmem),
        scratch_shapes=[
            pltpu.VMEM(forward.shape, jnp.bfloat16),
            pltpu.VMEM(taps.shape[1:], jnp.float32),
            pltpu.VMEM(filters.shape, jnp.float32),
            pltpu.SemaphoreType.DMA((rows // group + 3,)),
        ],
        compiler_params=pltpu.CompilerParams(vmem_limit_bytes=12 << 20),
    )(
        pltpu.with_memory_space_constraint(traces, pltpu.HBM),
        pltpu.with_memory_space_constraint(forward, pltpu.HBM),
        pltpu.with_memory_space_constraint(taps, pltpu.HBM),
        pltpu.with_memory_space_constraint(filters, pltpu.HBM),
    )


def last_kernel(m_ref, t_ref, i_ref, o_hbm, o_ref, sem, *, group, part):
    rows, cols, _ = t_ref.shape
    width = group * cols
    used = i_ref.shape[0]
    scale = 1.0 / math.sqrt(NF)

    def send(at):
        return pltpu.make_async_copy(o_ref.at[at], o_hbm.at[at], sem)

    for g in range(rows // group):
        m = m_ref[: used // 2, :, g * width : (g + 1) * width].reshape(used, width).T
        for h in range(group // part):
            acc = jnp.dot(
                m[h * part * cols : (h + 1) * part * cols], i_ref[...], preferred_element_type=jnp.float32
            )
            at = pl.ds(g * group + h * part, part)
            t = t_ref[at].astype(jnp.float32)
            o_ref[at] = (t - (acc * scale).reshape(t.shape)).astype(o_ref.dtype)
            send(at).start()
    pltpu.make_async_copy(o_ref, o_hbm, sem).wait()


def last(m, traces, inverse, group=8, part=2):
    vmem = pl.BlockSpec(memory_space=pltpu.VMEM)
    return pl.pallas_call(
        functools.partial(last_kernel, group=group, part=part),
        out_shape=jax.ShapeDtypeStruct(traces.shape, jnp.bfloat16),
        in_specs=[vmem, vmem, vmem],
        out_specs=pl.BlockSpec(memory_space=pltpu.HBM),
        scratch_shapes=[
            pltpu.VMEM(traces.shape, jnp.bfloat16),
            pltpu.SemaphoreType.DMA(()),
        ],
        compiler_params=pltpu.CompilerParams(vmem_limit_bytes=16 << 20),
    )(
        pltpu.with_memory_space_constraint(m, pltpu.VMEM),
        pltpu.with_memory_space_constraint(traces, pltpu.VMEM),
        inverse,
    )


def solution(mesh):
    n_freq, n_panel = mesh.shape["freq"], mesh.shape["panel"]
    n_all = n_freq * n_panel
    bins = FLO + np.arange(NF)
    cosine, sine = waves(bins, np.arange(NT))
    table = np.stack([cosine, -sine], 1).reshape(2 * NF, NT)
    forward = (table / math.sqrt(NT)).astype(np.float32).T
    inverse = table.astype(np.float32)
    tap_cos, tap_sin = waves(FLO + np.minimum(np.arange(n_all), NF - 1), np.arange(TAPS))
    taps = np.stack([tap_cos, -tap_sin], 1).astype(np.float32)

    def per_device(traces, filters):
        rows, cols, _ = traces.shape
        spectra, kept, reply = first(
            traces,
            jnp.asarray(forward, jnp.bfloat16),
            jnp.asarray(taps),
            filters.transpose(1, 0, 2),
            n_all,
            n_freq * cols,
        )
        slices = lax.all_to_all(spectra, BOTH, split_axis=0, concat_axis=0, tiled=True)
        matched = middle(slices, reply, n_freq, n_panel, rows, cols)
        back = lax.all_to_all(matched, BOTH, split_axis=0, concat_axis=0, tiled=True)
        return last(back, kept, jnp.asarray(inverse, jnp.bfloat16))

    placed = (P("panel", "freq", None), P())
    return jax.shard_map(
        per_device, mesh=mesh, in_specs=placed, out_specs=P("panel", "freq", None), check_vma=False
    )
```

```python
import functools
import math

import jax
import jax.numpy as jnp
import numpy as np
from jax import lax
from jax.experimental import pallas as pl
from jax.experimental.pallas import tpu as pltpu
from jax.sharding import PartitionSpec as P

NS = 640
NT = 1024
NF = 96
FLO = 8
TAPS = 64
SPAN = 7
RWIN = 40
NWIN = 16
BOTH = ("freq", "panel")


def waves(freq_bins, samples):
    phases = np.outer(freq_bins, samples) % NT
    angles = phases.astype(np.float64) * (2.0 * math.pi / NT)
    return np.cos(angles), np.sin(angles)


def exchange(parts, lane, unit):
    n, step = len(parts), 1
    while step < n:
        take = (lane // (unit * step)) % 2 == 1
        parts = [jnp.where(take, parts[(j + step) % n], parts[j]) for j in range(n)]
        step *= 2
    return parts


def mid_kernel(x_ref, w_ref, y_ref, z_ref, r_ref, o_ref, f_ref, xs_ref, *, n_freq, n_panel, rows, cols):
    f32, bf16 = jnp.float32, jnp.bfloat16
    pair = 2 * n_panel
    width = n_freq * cols
    tiles = width // 128
    unit = 128 // n_freq
    lane = lax.broadcasted_iota(jnp.int32, (pair, 128), 1)
    root = 1.0 / math.sqrt(NS)

    def words(q, g, u):
        return slice(q * pair, (q + 1) * pair), pl.ds(pl.multiple_of(g * width + u * 128, 128), 128)

    for q in range(n_freq):
        xs_ref[q * pair : (q + 1) * pair] = x_ref[q * n_panel : (q + 1) * n_panel].reshape(pair, rows * cols)

    def split(g, _):
        for u in range(tiles):
            sources = exchange([xs_ref[words(q, g, u)] for q in range(n_freq)], lane, unit)
            for s in range(n_freq):
                v = sources[-s % n_freq]
                v = pltpu.roll(v, 128 - s * unit, 1) if s else v
                z_ref[u, pl.ds(g * n_freq + s, pair, stride=rows), :] = v.astype(f32)
        return 0

    lax.fori_loop(0, rows // n_freq, split, 0)

    def place(q, _):
        for t in range(tiles):
            z = z_ref[t, pl.ds(pl.multiple_of(q * 4 * rows, 8), 4 * rows), :]
            re = jnp.concatenate([z[:rows], z[2 * rows : 3 * rows]], 0)
            im = jnp.concatenate([z[rows : 2 * rows], z[3 * rows :]], 0)
            c, d = slice(t * 128, t * 128 + 128), slice(width + t * 128, width + t * 128 + 128)
            for u in range(tiles):
                part = slice(u * unit, (u + 1) * unit)
                reb = re[part].astype(bf16)
                row = pl.multiple_of(u * 128 + q * unit, unit)
                r_ref[pl.ds(row, unit), c] = reb
                r_ref[pl.ds(row, unit), d] = im[part].astype(bf16)
                r_ref[pl.ds(row + NS, unit), c] = (-im[part]).astype(bf16)
                r_ref[pl.ds(row + NS, unit), d] = reb
        return 0

    lax.fori_loop(0, n_freq, place, 0)

    step = 256
    for n in range(2 * width // step):
        c = slice(n * step, n * step + step)
        o = jnp.dot(r_ref[:NS, :], r_ref[:, c], preferred_element_type=f32) * root
        for h in range(step // 128):
            t = n * (step // 128) + h
            ob = o[:, h * 128 : h * 128 + 128]
            o_ref[:NS, t * 128 : t * 128 + 128] = ob.astype(bf16)
            if t < tiles:
                o_ref[NS:, width + t * 128 : width + t * 128 + 128] = ob.astype(bf16)
            else:
                o_ref[NS:, (t - tiles) * 128 : (t - tiles) * 128 + 128] = (-ob).astype(bf16)
    zero = jnp.zeros((8, 128), f32)
    for t in range(3 * tiles):
        f_ref[t, 0:8, :] = zero
        f_ref[t, 8 + NS : 16 + NS, :] = zero
    for n in range(2 * width // step):
        c = slice(n * step, n * step + step)
        o = jnp.dot(r_ref[:NS, :], o_ref[:, c], preferred_element_type=f32) * root
        pred = (o_ref[:NS, c].astype(f32) - o).astype(bf16).astype(f32)
        for h in range(step // 128):
            t = n * (step // 128) + h
            for at in range(0, NS, unit):
                u, q = at // 128, at % 128 // unit
                dst = slice(8 + q * cols + u * unit, 8 + q * cols + (u + 1) * unit)
                v = pred[at : at + unit, h * 128 : h * 128 + 128]
                f_ref[t, dst, :] = v
                if t >= tiles:
                    f_ref[t + tiles, dst, :] = f_ref[t - tiles, dst, :] + v

    rim = SPAN // 2
    for t in range(tiles):
        weights = [
            jnp.broadcast_to(w_ref[i : i + 1, t * 128 : t * 128 + 128], (rows, 128)) for i in range(3 * SPAN)
        ]

        def match(p, _):
            sums = [None] * 3
            for j in range(SPAN):
                at = pl.ds(p * rows + 8 - rim + j, rows)
                for i, plane in enumerate((2 * tiles + t, tiles + t, t)):
                    term = weights[i * SPAN + j] * f_ref[plane, at, :]
                    sums[i] = term if sums[i] is None else sums[i] + term
            z_ref[t, pl.ds(pl.multiple_of(p * 2 * rows, 8), rows), :] = sums[0] - sums[1]
            z_ref[t, pl.ds(pl.multiple_of(p * 2 * rows + rows, 8), rows), :] = sums[0] + sums[2]
            return 0

        lax.fori_loop(0, n_panel, match, 0, unroll=4)

    def join(g, _):
        for u in range(tiles):
            sources = []
            for s in range(n_freq):
                v = z_ref[u, pl.ds(g * n_freq + s, pair, stride=rows), :].astype(bf16)
                sources.append(pltpu.roll(v, s * unit, 1) if s else v)
            blocks = exchange(sources, lane, unit)
            for q in range(n_freq):
                xs_ref[words(q, g, u)] = blocks[-q % n_freq]
        return 0

    lax.fori_loop(0, rows // n_freq, join, 0)
    for q in range(n_freq):
        y_ref[q * n_panel : (q + 1) * n_panel] = xs_ref[q * pair : (q + 1) * pair].reshape(
            n_panel, 2, rows * cols
        )


def middle(x, w, n_freq, n_panel, rows, cols):
    width = n_freq * cols
    f32, bf16 = jnp.float32, jnp.bfloat16
    return pl.pallas_call(
        functools.partial(mid_kernel, n_freq=n_freq, n_panel=n_panel, rows=rows, cols=cols),
        out_shape=pltpu.VMEM(x.shape, bf16),
        in_specs=[pl.BlockSpec(memory_space=pltpu.VMEM)] * 2,
        out_specs=pl.BlockSpec(memory_space=pltpu.VMEM),
        scratch_shapes=[
            pltpu.VMEM((width // 128, 2 * NS, 128), f32),
            pltpu.VMEM((2 * NS, 2 * width), bf16),
            pltpu.VMEM((2 * NS, 2 * width), bf16),
            pltpu.VMEM((3 * width // 128, NS + 16, 128), f32),
            pltpu.VMEM((2 * n_freq * n_panel, rows * cols), bf16),
        ],
        compiler_params=pltpu.CompilerParams(vmem_limit_bytes=26 << 20),
    )(
        pltpu.with_memory_space_constraint(x, pltpu.VMEM),
        pltpu.with_memory_space_constraint(w, pltpu.VMEM),
    )


def first_kernel(t_hbm, f_hbm, tap_hbm, filt_hbm, s_ref, t_ref, w_ref, f_ref, tap_ref, filt_ref, sem, *, group):
    rows, cols, _ = t_ref.shape
    width, unit = group * cols, 128 // group
    used = f_ref.shape[1] // 2
    block = lax.axis_index("freq")

    def fetch(g):
        at = pl.ds(g * group, group)
        return pltpu.make_async_copy(t_hbm.at[at], t_ref.at[at], sem.at[g])

    table = pltpu.make_async_copy(f_hbm, f_ref, sem.at[rows // group])
    tap = pltpu.make_async_copy(tap_hbm.at[lax.axis_index(BOTH)], tap_ref, sem.at[rows // group + 1])
    filt = pltpu.make_async_copy(filt_hbm, filt_ref, sem.at[rows // group + 2])
    tap.start()
    filt.start()
    table.start()
    for g in range(rows // group):
        fetch(g).start()
    s_ref[used:] = jnp.zeros((s_ref.shape[0] - used,) + s_ref.shape[1:], s_ref.dtype)
    tap.wait()
    filt.wait()
    window = lax.broadcasted_iota(jnp.int32, (NWIN, w_ref.shape[1]), 0) * RWIN
    place = lax.broadcasted_iota(jnp.int32, (NWIN, w_ref.shape[1]), 1)
    place = (place % 128) // unit * cols + place // 128 * unit + place % unit - window
    inside = (place >= 0) & (place < RWIN)
    for j in range(SPAN):
        real, imag = (
            jnp.sum(
                jnp.where(inside, jnp.sum(filt_ref[j] * tap_ref[c : c + 1, :], 1, keepdims=True), 0.0),
                0,
                keepdims=True,
            )
            for c in range(2)
        )
        w_ref[j : j + 1, :] = real
        w_ref[SPAN + j : SPAN + j + 1, :] = real + imag
        w_ref[2 * SPAN + j : 2 * SPAN + j + 1, :] = imag - real
    table.wait()
    for g in range(rows // group):
        fetch(g).wait()
        pieces = [
            t_ref[g * group + (k + group - block) % group, u * unit : (u + 1) * unit]
            for u in range(cols // unit)
            for k in range(group)
        ]
        half = len(pieces) // 2
        out = jnp.concatenate(
            [
                jnp.dot(jnp.concatenate(part, 0), f_ref[...], preferred_element_type=jnp.float32)
                for part in (pieces[:half], pieces[half:])
            ],
            0,
        )
        s_ref[:used, :, g * width : (g + 1) * width] = out.astype(s_ref.dtype).T.reshape(used, 2, width)


def first(traces, forward, taps, filters, n_all, receivers, group=8):
    rows, cols, _ = traces.shape
    hbm, vmem = pl.BlockSpec(memory_space=pltpu.HBM), pl.BlockSpec(memory_space=pltpu.VMEM)
    return pl.pallas_call(
        functools.partial(first_kernel, group=group),
        out_shape=(
            pltpu.VMEM((n_all, 2, rows * cols), jnp.bfloat16),
            pltpu.VMEM(traces.shape, jnp.bfloat16),
            pltpu.VMEM((3 * SPAN, receivers), jnp.float32),
        ),
        in_specs=[hbm] * 4,
        out_specs=(vmem, vmem, vmem),
        scratch_shapes=[
            pltpu.VMEM(forward.shape, jnp.bfloat16),
            pltpu.VMEM(taps.shape[1:], jnp.float32),
            pltpu.VMEM(filters.shape, jnp.float32),
            pltpu.SemaphoreType.DMA((rows // group + 3,)),
        ],
        compiler_params=pltpu.CompilerParams(vmem_limit_bytes=12 << 20),
    )(
        pltpu.with_memory_space_constraint(traces, pltpu.HBM),
        pltpu.with_memory_space_constraint(forward, pltpu.HBM),
        pltpu.with_memory_space_constraint(taps, pltpu.HBM),
        pltpu.with_memory_space_constraint(filters, pltpu.HBM),
    )


def last_kernel(m_ref, t_ref, i_ref, o_hbm, o_ref, sem, *, group, part):
    rows, cols, _ = t_ref.shape
    width, unit = group * cols, 128 // group
    used = i_ref.shape[0]
    block = lax.axis_index("freq")
    scale = 1.0 / math.sqrt(NF)

    def send(at):
        return pltpu.make_async_copy(o_ref.at[at], o_hbm.at[at], sem)

    for g in range(rows // group):
        m = m_ref[: used // 2, :, g * width : (g + 1) * width].reshape(used, width).T
        for h in range(0, group, part):
            pieces = [
                m[u * 128 + k * unit : u * 128 + (k + 1) * unit]
                for k in range(h, h + part)
                for u in range(cols // unit)
            ]
            acc = jnp.dot(jnp.concatenate(pieces, 0), i_ref[...], preferred_element_type=jnp.float32)
            for k in range(part):
                at = g * group + (h + k + group - block) % group
                t = t_ref[at].astype(jnp.float32)
                o_ref[at] = (t - acc[k * cols : (k + 1) * cols] * scale).astype(o_ref.dtype)
                send(at).start()
    pltpu.make_async_copy(o_ref, o_hbm, sem).wait()


def last(m, traces, inverse, group=8, part=2):
    vmem = pl.BlockSpec(memory_space=pltpu.VMEM)
    return pl.pallas_call(
        functools.partial(last_kernel, group=group, part=part),
        out_shape=jax.ShapeDtypeStruct(traces.shape, jnp.bfloat16),
        in_specs=[vmem, vmem, vmem],
        out_specs=pl.BlockSpec(memory_space=pltpu.HBM),
        scratch_shapes=[
            pltpu.VMEM(traces.shape, jnp.bfloat16),
            pltpu.SemaphoreType.DMA(()),
        ],
        compiler_params=pltpu.CompilerParams(vmem_limit_bytes=16 << 20),
    )(
        pltpu.with_memory_space_constraint(m, pltpu.VMEM),
        pltpu.with_memory_space_constraint(traces, pltpu.VMEM),
        inverse,
    )


def solution(mesh):
    n_freq, n_panel = mesh.shape["freq"], mesh.shape["panel"]
    n_all = n_freq * n_panel
    bins = FLO + np.arange(NF)
    cosine, sine = waves(bins, np.arange(NT))
    table = np.stack([cosine, -sine], 1).reshape(2 * NF, NT)
    forward = (table / math.sqrt(NT)).astype(np.float32).T
    inverse = table.astype(np.float32)
    tap_cos, tap_sin = waves(FLO + np.minimum(np.arange(n_all), NF - 1), np.arange(TAPS))
    taps = np.stack([tap_cos, -tap_sin], 1).astype(np.float32)

    def per_device(traces, filters):
        rows, cols, _ = traces.shape
        spectra, kept, reply = first(
            traces,
            jnp.asarray(forward, jnp.bfloat16),
            jnp.asarray(taps),
            filters.transpose(1, 0, 2),
            n_all,
            n_freq * cols,
        )
        slices = lax.all_to_all(spectra, BOTH, split_axis=0, concat_axis=0, tiled=True)
        matched = middle(slices, reply, n_freq, n_panel, rows, cols)
        back = lax.all_to_all(matched, BOTH, split_axis=0, concat_axis=0, tiled=True)
        return last(back, kept, jnp.asarray(inverse, jnp.bfloat16))

    placed = (P("panel", "freq", None), P())
    return jax.shard_map(
        per_device, mesh=mesh, in_specs=placed, out_specs=P("panel", "freq", None), check_vma=False
    )
```

```python
import functools
import math

import jax
import jax.numpy as jnp
import numpy as np
from jax import lax
from jax.experimental import pallas as pl
from jax.experimental.pallas import tpu as pltpu
from jax.sharding import PartitionSpec as P

NS = 640
NT = 1024
NF = 96
FLO = 8
TAPS = 64
SPAN = 7
RWIN = 40
NWIN = 16
BOTH = ("freq", "panel")


def waves(freq_bins, samples):
    phases = np.outer(freq_bins, samples) % NT
    angles = phases.astype(np.float64) * (2.0 * math.pi / NT)
    return np.cos(angles), np.sin(angles)


def exchange(parts, lane, unit):
    n, step = len(parts), 1
    while step < n:
        take = (lane // (unit * step)) % 2 == 1
        parts = [jnp.where(take, parts[(j + step) % n], parts[j]) for j in range(n)]
        step *= 2
    return parts


def mid_kernel(x_ref, w_ref, y_ref, z_ref, r_ref, o_ref, f_ref, xs_ref, *, n_freq, n_panel, rows, cols):
    f32, bf16 = jnp.float32, jnp.bfloat16
    pair = 2 * n_panel
    width = n_freq * cols
    tiles = width // 128
    unit = 128 // n_freq
    lane = lax.broadcasted_iota(jnp.int32, (pair, 128), 1)
    root = 1.0 / math.sqrt(NS)

    def words(q, g, u):
        return slice(q * pair, (q + 1) * pair), pl.ds(pl.multiple_of(g * width + u * 128, 128), 128)

    for q in range(n_freq):
        xs_ref[q * pair : (q + 1) * pair] = x_ref[q * n_panel : (q + 1) * n_panel].reshape(pair, rows * cols)

    def split(g, _):
        for u in range(tiles):
            sources = exchange([xs_ref[words(q, g, u)] for q in range(n_freq)], lane, unit)
            for s in range(n_freq):
                v = sources[-s % n_freq]
                v = pltpu.roll(v, 128 - s * unit, 1) if s else v
                z_ref[u, pl.ds(g * n_freq + s, pair, stride=rows), :] = v.astype(f32)
        return 0

    lax.fori_loop(0, rows // n_freq, split, 0)

    def place(q, _):
        for t in range(tiles):
            z = z_ref[t, pl.ds(pl.multiple_of(q * 4 * rows, 8), 4 * rows), :]
            re = jnp.concatenate([z[:rows], z[2 * rows : 3 * rows]], 0)
            im = jnp.concatenate([z[rows : 2 * rows], z[3 * rows :]], 0)
            c, d = slice(t * 128, t * 128 + 128), slice(width + t * 128, width + t * 128 + 128)
            for u in range(tiles):
                part = slice(u * unit, (u + 1) * unit)
                reb = re[part].astype(bf16)
                row = pl.multiple_of(u * 128 + q * unit, unit)
                r_ref[pl.ds(row, unit), c] = reb
                r_ref[pl.ds(row, unit), d] = im[part].astype(bf16)
                r_ref[pl.ds(row + NS, unit), c] = (-im[part]).astype(bf16)
                r_ref[pl.ds(row + NS, unit), d] = reb
        return 0

    lax.fori_loop(0, n_freq, place, 0)

    step = 256
    for n in range(2 * width // step):
        c = slice(n * step, n * step + step)
        o = jnp.dot(r_ref[:NS, :], r_ref[:, c], preferred_element_type=f32) * root
        for h in range(step // 128):
            t = n * (step // 128) + h
            ob = o[:, h * 128 : h * 128 + 128]
            o_ref[:NS, t * 128 : t * 128 + 128] = ob.astype(bf16)
            if t < tiles:
                o_ref[NS:, width + t * 128 : width + t * 128 + 128] = ob.astype(bf16)
            else:
                o_ref[NS:, (t - tiles) * 128 : (t - tiles) * 128 + 128] = (-ob).astype(bf16)
    zero = jnp.zeros((8, 128), f32)
    for t in range(3 * tiles):
        f_ref[t, 0:8, :] = zero
        f_ref[t, 8 + NS : 16 + NS, :] = zero
    for n in range(2 * width // step):
        c = slice(n * step, n * step + step)
        o = jnp.dot(r_ref[:NS, :], o_ref[:, c], preferred_element_type=f32) * root
        pred = (o_ref[:NS, c].astype(f32) - o).astype(bf16).astype(f32)
        for h in range(step // 128):
            t = n * (step // 128) + h
            for at in range(0, NS, unit):
                u, q = at // 128, at % 128 // unit
                dst = slice(8 + q * cols + u * unit, 8 + q * cols + (u + 1) * unit)
                v = pred[at : at + unit, h * 128 : h * 128 + 128]
                f_ref[t, dst, :] = v
                if t >= tiles:
                    f_ref[t + tiles, dst, :] = f_ref[t - tiles, dst, :] + v

    rim = SPAN // 2
    for t in range(tiles):
        weights = [
            jnp.broadcast_to(w_ref[i : i + 1, t * 128 : t * 128 + 128], (rows, 128)) for i in range(3 * SPAN)
        ]

        def match(p, _):
            sums = [None] * 3
            for j in range(SPAN):
                at = pl.ds(p * rows + 8 - rim + j, rows)
                for i, plane in enumerate((2 * tiles + t, tiles + t, t)):
                    term = weights[i * SPAN + j] * f_ref[plane, at, :]
                    sums[i] = term if sums[i] is None else sums[i] + term
            z_ref[t, pl.ds(pl.multiple_of(p * 2 * rows, 8), rows), :] = sums[0] - sums[1]
            z_ref[t, pl.ds(pl.multiple_of(p * 2 * rows + rows, 8), rows), :] = sums[0] + sums[2]
            return 0

        lax.fori_loop(0, n_panel, match, 0, unroll=4)

    def join(g, _):
        for u in range(tiles):
            sources = []
            for s in range(n_freq):
                v = z_ref[u, pl.ds(g * n_freq + s, pair, stride=rows), :].astype(bf16)
                sources.append(pltpu.roll(v, s * unit, 1) if s else v)
            blocks = exchange(sources, lane, unit)
            for q in range(n_freq):
                xs_ref[words(q, g, u)] = blocks[-q % n_freq]
        return 0

    lax.fori_loop(0, rows // n_freq, join, 0)
    for q in range(n_freq):
        y_ref[q * n_panel : (q + 1) * n_panel] = xs_ref[q * pair : (q + 1) * pair].reshape(
            n_panel, 2, rows * cols
        )


def middle(x, w, n_freq, n_panel, rows, cols):
    width = n_freq * cols
    f32, bf16 = jnp.float32, jnp.bfloat16
    return pl.pallas_call(
        functools.partial(mid_kernel, n_freq=n_freq, n_panel=n_panel, rows=rows, cols=cols),
        out_shape=pltpu.VMEM(x.shape, bf16),
        in_specs=[pl.BlockSpec(memory_space=pltpu.VMEM)] * 2,
        out_specs=pl.BlockSpec(memory_space=pltpu.VMEM),
        scratch_shapes=[
            pltpu.VMEM((width // 128, 2 * NS, 128), f32),
            pltpu.VMEM((2 * NS, 2 * width), bf16),
            pltpu.VMEM((2 * NS, 2 * width), bf16),
            pltpu.VMEM((3 * width // 128, NS + 16, 128), f32),
            pltpu.VMEM((2 * n_freq * n_panel, rows * cols), bf16),
        ],
        compiler_params=pltpu.CompilerParams(vmem_limit_bytes=26 << 20),
    )(
        pltpu.with_memory_space_constraint(x, pltpu.VMEM),
        pltpu.with_memory_space_constraint(w, pltpu.VMEM),
    )


def first_kernel(t_hbm, f_hbm, tap_hbm, filt_hbm, s_ref, t_ref, w_ref, f_ref, tap_ref, filt_ref, sem, *, group):
    rows, cols, _ = t_ref.shape
    width, unit = group * cols, 128 // group
    used = f_ref.shape[1] // 2
    scale = 1.0 / math.sqrt(NF)
    block = lax.axis_index("freq")

    def fetch(g):
        at = pl.ds(g * group, group)
        return pltpu.make_async_copy(t_hbm.at[at], t_ref.at[at], sem.at[g])

    table = pltpu.make_async_copy(f_hbm, f_ref, sem.at[rows // group])
    tap = pltpu.make_async_copy(tap_hbm.at[lax.axis_index(BOTH)], tap_ref, sem.at[rows // group + 1])
    filt = pltpu.make_async_copy(filt_hbm, filt_ref, sem.at[rows // group + 2])
    tap.start()
    filt.start()
    table.start()
    for g in range(rows // group):
        fetch(g).start()
    s_ref[used:] = jnp.zeros((s_ref.shape[0] - used,) + s_ref.shape[1:], s_ref.dtype)
    tap.wait()
    filt.wait()
    window = lax.broadcasted_iota(jnp.int32, (NWIN, w_ref.shape[1]), 0) * RWIN
    place = lax.broadcasted_iota(jnp.int32, (NWIN, w_ref.shape[1]), 1)
    place = (place % 128) // unit * cols + place // 128 * unit + place % unit - window
    inside = (place >= 0) & (place < RWIN)
    for j in range(SPAN):
        real, imag = (
            jnp.sum(
                jnp.where(inside, jnp.sum(filt_ref[j] * tap_ref[c : c + 1, :], 1, keepdims=True), 0.0),
                0,
                keepdims=True,
            )
            for c in range(2)
        )
        real, imag = real * scale, imag * scale
        w_ref[j : j + 1, :] = real
        w_ref[SPAN + j : SPAN + j + 1, :] = real + imag
        w_ref[2 * SPAN + j : 2 * SPAN + j + 1, :] = imag - real
    table.wait()
    for g in range(rows // group):
        fetch(g).wait()
        pieces = [
            t_ref[g * group + (k + group - block) % group, u * unit : (u + 1) * unit]
            for u in range(cols // unit)
            for k in range(group)
        ]
        half = len(pieces) // 2
        out = jnp.concatenate(
            [
                jnp.dot(jnp.concatenate(part, 0), f_ref[...], preferred_element_type=jnp.float32)
                for part in (pieces[:half], pieces[half:])
            ],
            0,
        )
        s_ref[:used, :, g * width : (g + 1) * width] = out.astype(s_ref.dtype).T.reshape(used, 2, width)


def first(traces, forward, taps, filters, n_all, receivers, group=8):
    rows, cols, _ = traces.shape
    hbm, vmem = pl.BlockSpec(memory_space=pltpu.HBM), pl.BlockSpec(memory_space=pltpu.VMEM)
    return pl.pallas_call(
        functools.partial(first_kernel, group=group),
        out_shape=(
            pltpu.VMEM((n_all, 2, rows * cols), jnp.bfloat16),
            pltpu.VMEM(traces.shape, jnp.bfloat16),
            pltpu.VMEM((3 * SPAN, receivers), jnp.float32),
        ),
        in_specs=[hbm] * 4,
        out_specs=(vmem, vmem, vmem),
        scratch_shapes=[
            pltpu.VMEM(forward.shape, jnp.bfloat16),
            pltpu.VMEM(taps.shape[1:], jnp.float32),
            pltpu.VMEM(filters.shape, jnp.float32),
            pltpu.SemaphoreType.DMA((rows // group + 3,)),
        ],
        compiler_params=pltpu.CompilerParams(vmem_limit_bytes=12 << 20),
    )(
        pltpu.with_memory_space_constraint(traces, pltpu.HBM),
        pltpu.with_memory_space_constraint(forward, pltpu.HBM),
        pltpu.with_memory_space_constraint(taps, pltpu.HBM),
        pltpu.with_memory_space_constraint(filters, pltpu.HBM),
    )


def last_kernel(m_ref, t_ref, i_ref, o_hbm, o_ref, sem, *, group, part):
    rows, cols, _ = t_ref.shape
    width, unit = group * cols, 128 // group
    used = i_ref.shape[0]
    block = lax.axis_index("freq")

    def send(at):
        return pltpu.make_async_copy(o_ref.at[at], o_hbm.at[at], sem)

    for g in range(rows // group):
        m = m_ref[: used // 2, :, g * width : (g + 1) * width].reshape(used, width).T
        for h in range(0, group, part):
            pieces = [
                m[u * 128 + k * unit : u * 128 + (k + 1) * unit]
                for k in range(h, h + part)
                for u in range(cols // unit)
            ]
            acc = jnp.dot(jnp.concatenate(pieces, 0), i_ref[...], preferred_element_type=jnp.float32)
            for k in range(part):
                at = g * group + (h + k + group - block) % group
                t = t_ref[at].astype(jnp.float32)
                o_ref[at] = (t - acc[k * cols : (k + 1) * cols]).astype(o_ref.dtype)
                send(at).start()
    pltpu.make_async_copy(o_ref, o_hbm, sem).wait()


def last(m, traces, inverse, group=8, part=2):
    vmem = pl.BlockSpec(memory_space=pltpu.VMEM)
    return pl.pallas_call(
        functools.partial(last_kernel, group=group, part=part),
        out_shape=jax.ShapeDtypeStruct(traces.shape, jnp.bfloat16),
        in_specs=[vmem, vmem, vmem],
        out_specs=pl.BlockSpec(memory_space=pltpu.HBM),
        scratch_shapes=[
            pltpu.VMEM(traces.shape, jnp.bfloat16),
            pltpu.SemaphoreType.DMA(()),
        ],
        compiler_params=pltpu.CompilerParams(vmem_limit_bytes=16 << 20),
    )(
        pltpu.with_memory_space_constraint(m, pltpu.VMEM),
        pltpu.with_memory_space_constraint(traces, pltpu.VMEM),
        inverse,
    )


def solution(mesh):
    n_freq, n_panel = mesh.shape["freq"], mesh.shape["panel"]
    n_all = n_freq * n_panel
    bins = FLO + np.arange(NF)
    cosine, sine = waves(bins, np.arange(NT))
    table = np.stack([cosine, -sine], 1).reshape(2 * NF, NT)
    forward = (table / math.sqrt(NT)).astype(np.float32).T
    inverse = table.astype(np.float32)
    tap_cos, tap_sin = waves(FLO + np.minimum(np.arange(n_all), NF - 1), np.arange(TAPS))
    taps = np.stack([tap_cos, -tap_sin], 1).astype(np.float32)

    def per_device(traces, filters):
        rows, cols, _ = traces.shape
        spectra, kept, reply = first(
            traces,
            jnp.asarray(forward, jnp.bfloat16),
            jnp.asarray(taps),
            filters.transpose(1, 0, 2),
            n_all,
            n_freq * cols,
        )
        slices = lax.all_to_all(spectra, BOTH, split_axis=0, concat_axis=0, tiled=True)
        matched = middle(slices, reply, n_freq, n_panel, rows, cols)
        back = lax.all_to_all(matched, BOTH, split_axis=0, concat_axis=0, tiled=True)
        return last(back, kept, jnp.asarray(inverse, jnp.bfloat16))

    placed = (P("panel", "freq", None), P())
    return jax.shard_map(
        per_device, mesh=mesh, in_specs=placed, out_specs=P("panel", "freq", None), check_vma=False
    )
```
